512 devices in a mesh: tm: 16 (over x_lo, y), stn: 32 (over x_hi, z, core).
Axes of the slice: x: 4 (x_hi: 2, x_lo: 2; x = x_hi * 2 + x_lo), y: 8, z: 8, core: 2. Of those that a mesh axis runs over, the one named last changes fastest.
Arguments:
- voltages: bfloat16 [2, 1024, 65536], P(None, 'stn', 'tm'), may hold values from -6 to 6
- filter_taps: float32 [12, 4096], replicated, may hold values from -1.75 to 1.75
- beam_weights: int32 [2, 512, 1024], P(None, 'stn'), may hold values from -32768 to 32767
- station_map: int32 [512], replicated, may hold values from 0 to 511, each once
- station_flags: int32 [512], replicated, may hold values 0 or 1
Outputs:
- beam_power: float32 [512, 16, 4096], P('stn', 'tm')
The draws below stay inside these ranges and needn't reach their ends.
Inputs may be any that keep to these rules, and one draw needn't show every extreme that they name: `station_map`: each station number appears once.
All inputs are finite; a program needn't handle non-finite values.
Results may differ from the reference program's by a relative error of at most 0.0039.
Values may be sent and summed in bfloat16 or wider, within the bound.
No kernel may reach another device: no remote copies, remote signals or barrier semaphores. Data moves between devices by JAX's collectives and lax.ppermute only.
A program may use at most 64 MiB of HBM per device.

```python
import jax
import jax.numpy as jnp
from jax import lax

S = 512
B = 512
C = 4096
TAPS = 12
NIN = 1024
NFR = 16


def with_ends(values, own_key, low, high):
    longest = values.shape.index(max(values.shape))
    spots = []
    for shift in (0, 1):
        where = [jax.random.randint(jax.random.fold_in(own_key, axis), (), 0, length) for axis, length in enumerate(values.shape)]
        where[longest] = (where[longest] + shift) % values.shape[longest]
        spots.append(tuple(where))
    return values.at[spots[0]].set(low).at[spots[1]].set(high)


def level_of(own_key, extent, cuts, low, top_value):
    loudness = 1.0
    for dim, parts in cuts:
        steps = jax.random.uniform(jax.random.fold_in(jax.random.fold_in(own_key, 6), dim), (parts,), jnp.float32, low / len(cuts), top_value / len(cuts))
        loudness = loudness * jnp.repeat(jnp.exp(steps), extent[dim] // parts).reshape((-1,) + (1,) * (len(extent) - 1 - dim))
    return loudness


def gaussian(rng, shape, scale, bound, shards=(), held_as=jnp.bfloat16):
    array = jax.random.normal(rng, shape, jnp.float32) * scale
    if len(shards) > 0:
        array = level_of(rng, shape, shards, -0.22, 0.18) * array
    return jnp.clip(array, min=-bound, max=bound).astype(held_as)


def setup_inputs(seed: int = 0) -> dict:
    key_of = jax.random.split(jax.random.key(seed), 6)
    voltages = gaussian(key_of[0], (2, NIN, NFR * C), 1.0, 6.0, ((1, 32), (2, 16)))
    filter_taps = gaussian(key_of[1], (TAPS, C), TAPS ** -0.5, 1.75, (), jnp.float32)
    beam_weights = with_ends(jax.random.randint(key_of[2], (2, B, NIN), -32768, 32768), jax.random.fold_in(key_of[2], 1), -32768, 32767).astype(jnp.int32)
    station_map = jax.random.permutation(key_of[3], S).astype(jnp.int32)
    station_flags = with_ends((jax.random.randint(key_of[4], (S,), 0, 8) < 7).astype(jnp.int32), jax.random.fold_in(key_of[4], 1), 0, 1)
    return dict(voltages=voltages, filter_taps=filter_taps, beam_weights=beam_weights, station_map=station_map, station_flags=station_flags)


def reference(voltages, filter_taps, beam_weights, station_map, station_flags):
    flag_slot = station_flags[station_map]
    keep_mask = jnp.repeat(flag_slot, 2).astype(voltages.dtype)
    masked = voltages * keep_mask[None, :, None]
    frames = masked.reshape(2, NIN, NFR, C)
    padded = jnp.concatenate([jnp.zeros((2, NIN, TAPS - 1, C), frames.dtype), frames], axis=2)
    weight_int = beam_weights.reshape(2, B, S, 2)[:, :, station_map, :].reshape(2, B, NIN)
    weight_low = (weight_int.astype(jnp.float32) * (1.0 / 32768.0)).astype(jnp.bfloat16)
    weight_full = lax.optimization_barrier(weight_low).astype(jnp.float32)

    def per_frame(frame_index):
        window = lax.dynamic_slice_in_dim(padded, frame_index, TAPS, 2).astype(jnp.float32)
        filtered = lax.optimization_barrier(jnp.sum(window * filter_taps[None, None, :, :], axis=2))
        spectrum = jnp.fft.fft(lax.complex(filtered[0], filtered[1]), axis=-1) / jnp.sqrt(jnp.float32(C))
        chan_real = lax.optimization_barrier(jnp.real(spectrum).astype(jnp.bfloat16)).astype(jnp.float32)
        chan_imag = lax.optimization_barrier(jnp.imag(spectrum).astype(jnp.bfloat16)).astype(jnp.float32)
        beam_real = jnp.dot(weight_full[0], chan_real) - jnp.dot(weight_full[1], chan_imag)
        beam_imag = jnp.dot(weight_full[0], chan_imag) + jnp.dot(weight_full[1], chan_real)
        return (beam_real * beam_real + beam_imag * beam_imag) / NIN
    power_all = lax.map(per_frame, jnp.arange(NFR, dtype=jnp.int32))
    return jnp.transpose(power_all, (1, 0, 2))
```

```python
import math

import jax
import jax.numpy as jnp
from jax import lax
from jax.sharding import PartitionSpec as P

RADIX = 64


exact_mode = lax.Precision.HIGHEST

BOTH = ("tm", "stn")


def stn_index(xhi, z, core):
    return xhi * 16 + z * 2 + core


Z_GROUPS = [[stn_index(xhi, z, core) for z in range(8)] for xhi in range(2) for core in range(2)]
SWAP_XHI = [(i, i ^ 16) for i in range(32)]
SWAP_CORE = [(i, i ^ 1) for i in range(32)]


def transform(real_in, imag_in, channels):
    index_row = jnp.arange(RADIX, dtype=jnp.int32)
    product = index_row[:, None] * index_row[None, :]
    angle_table = (product % RADIX).astype(jnp.float32) * (2.0 * math.pi / RADIX)
    cosine = jnp.cos(angle_table)
    sine_part = jnp.sin(angle_table)
    twiddle = product.astype(jnp.float32) * (2.0 * math.pi / channels)
    twiddle_cos = jnp.cos(twiddle)
    twiddle_sin = jnp.sin(twiddle)
    batch_rows = real_in.shape[0]
    real_cube = real_in.reshape(batch_rows, RADIX, RADIX)
    imag_cube = imag_in.reshape(batch_rows, RADIX, RADIX)
    mid_real = jnp.einsum("pab,ak->pbk", real_cube, cosine, precision=exact_mode) + jnp.einsum(
        "pab,ak->pbk", imag_cube, sine_part, precision=exact_mode
    )
    mid_imag = jnp.einsum("pab,ak->pbk", imag_cube, cosine, precision=exact_mode) - jnp.einsum(
        "pab,ak->pbk", real_cube, sine_part, precision=exact_mode
    )
    turn_real = mid_real * twiddle_cos + mid_imag * twiddle_sin
    turn_imag = mid_imag * twiddle_cos - mid_real * twiddle_sin
    out_real = jnp.einsum("pbk,bm->pmk", turn_real, cosine, precision=exact_mode) + jnp.einsum(
        "pbk,bm->pmk", turn_imag, sine_part, precision=exact_mode
    )
    out_imag = jnp.einsum("pbk,bm->pmk", turn_imag, cosine, precision=exact_mode) - jnp.einsum(
        "pbk,bm->pmk", turn_real, sine_part, precision=exact_mode
    )
    norm_scale = 1.0 / math.sqrt(channels)
    return (
        out_real.reshape(batch_rows, channels) * norm_scale,
        out_imag.reshape(batch_rows, channels) * norm_scale,
    )


def filter_spectra(extended, filter_taps, frame_count):
    inputs_here = extended.shape[1]
    channels = extended.shape[3]
    filtered = jnp.zeros((2, inputs_here, frame_count, channels), jnp.float32)
    for tap_index in range(filter_taps.shape[0]):
        filtered = filtered + filter_taps[tap_index] * extended[
            :, :, tap_index : tap_index + frame_count
        ].astype(jnp.float32)
    chan_real, chan_imag = transform(
        filtered[0].reshape(-1, channels), filtered[1].reshape(-1, channels), channels
    )
    return jnp.stack([chan_real.astype(jnp.bfloat16), chan_imag.astype(jnp.bfloat16)]).reshape(
        2, inputs_here, frame_count, channels
    )


def local_weights(beam_weights, station_map, station_flags):
    beams = beam_weights.shape[1]
    inputs = beam_weights.shape[2]
    order = station_map.reshape(32, 16).T.reshape(-1)
    target = (2 * order[:, None] + jnp.arange(2, dtype=jnp.int32)[None, :]).reshape(-1)
    keep = jnp.repeat(station_flags, 2)
    rows = jnp.arange(inputs, dtype=jnp.int32)
    select = ((rows[:, None] == target[None, :]) & (keep[:, None] > 0)).astype(jnp.bfloat16)
    weight_low = (beam_weights.astype(jnp.float32) * (1.0 / 32768.0)).astype(jnp.bfloat16)
    return jnp.dot(
        weight_low.reshape(2 * beams, inputs), select, preferred_element_type=jnp.float32
    ).astype(jnp.bfloat16)


def block_power(weights, spectra, inputs_all):
    product = jnp.dot(weights, spectra, preferred_element_type=jnp.float32)
    product = product.reshape(8, 2, 16, 2, 128)
    beam_real = product[:, 0, :, 0] - product[:, 1, :, 1]
    beam_imag = product[:, 0, :, 1] + product[:, 1, :, 0]
    return ((beam_real * beam_real + beam_imag * beam_imag) / inputs_all).astype(jnp.bfloat16)


def on_device(voltages, filter_taps, beam_weights, station_map, station_flags):
    channels = filter_taps.shape[1]
    history = filter_taps.shape[0] - 1
    inputs_all = beam_weights.shape[2]
    retiled = lax.all_to_all(voltages, "tm", split_axis=1, concat_axis=2, tiled=True)
    own = local_weights(beam_weights, station_map, station_flags)
    gathered = lax.all_gather(own, "stn", axis=0, tiled=True, axis_index_groups=Z_GROUPS)
    few_inputs = retiled.shape[1]
    all_frames = retiled.shape[2] // channels
    frames = retiled.reshape(2, few_inputs, all_frames, channels)
    extended = jnp.concatenate(
        [jnp.zeros((2, few_inputs, history, channels), frames.dtype), frames], axis=2
    )
    spectra = filter_spectra(extended, filter_taps, all_frames)
    outgoing = spectra.reshape(2, 2, 16, 32, 128).transpose(2, 3, 1, 0, 4).reshape(512, 2, 256)
    turned = lax.all_to_all(outgoing, BOTH, split_axis=0, concat_axis=0, tiled=True)
    turned = turned.reshape(inputs_all, 256)
    other_core = lax.ppermute(gathered, "stn", SWAP_CORE)
    other_xhi = lax.ppermute(gathered, "stn", SWAP_XHI)
    other_both = lax.ppermute(other_xhi, "stn", SWAP_CORE)
    power = jnp.stack(
        [
            jnp.stack([block_power(gathered, turned, inputs_all), block_power(other_core, turned, inputs_all)], 1),
            jnp.stack([block_power(other_xhi, turned, inputs_all), block_power(other_both, turned, inputs_all)], 1),
        ]
    )
    here = lax.axis_index("stn")
    power = jnp.where(here % 2 == 1, power[:, :, ::-1], power)
    power = jnp.where(here >= 16, power[::-1], power)
    received = lax.all_to_all(power.reshape(32, 16, 128), "stn", 0, 0, tiled=True)
    return received.transpose(1, 0, 2).reshape(16, 1, channels).astype(jnp.float32)


def solution(mesh):
    placed = (P(None, "stn", "tm"), P(), P(None, "stn", None), P(), P())
    return jax.shard_map(
        on_device, mesh=mesh, in_specs=placed, out_specs=P("stn", "tm", None), check_vma=False
    )
```

```python
import math

import jax
import jax.numpy as jnp
import numpy as np
from jax import lax
from jax.experimental import pallas as pl
from jax.experimental.pallas import tpu as pltpu
from jax.sharding import PartitionSpec as P

BOTH = ("tm", "stn")
LANES = 128
FRAMES = 16
OUTER = 32
TAPS = 12


def stn_index(xhi, z, core):
    return xhi * 16 + z * 2 + core


QUADS = [
    [stn_index(xhi, 4 * half + z, core) for z in range(4)]
    for xhi in range(2)
    for half in range(2)
    for core in range(2)
]
SWAP_XHI = [(i, i ^ 16) for i in range(32)]
SWAP_HALF = [(i, i ^ 8) for i in range(32)]
SWAP_CORE = [(i, i ^ 1) for i in range(32)]


def dft_tables(channels):
    b = np.arange(LANES, dtype=np.float64)
    k1 = np.arange(OUTER, dtype=np.float64)
    turn = 2.0 * np.pi * k1[:, None] * b[None, :] / channels
    twiddle = np.stack([np.cos(turn), np.sin(turn)]).astype(np.float32)
    inner = 2.0 * np.pi * ((b[:, None] * b[None, :]) % LANES) / LANES
    scale = 1.0 / math.sqrt(channels)
    table = (np.concatenate([np.cos(inner), np.sin(inner)]) * scale).astype(np.float32)
    return twiddle, table


def times(value, angle):
    real, imag = value
    cosine, sine = math.cos(angle), math.sin(angle)
    if abs(sine) < 1e-12:
        return (real, imag) if cosine > 0 else (-real, -imag)
    if abs(cosine) < 1e-12:
        return (imag, -real) if sine > 0 else (-imag, real)
    if abs(abs(cosine) - abs(sine)) < 1e-12:
        sign_c = 1.0 if cosine > 0 else -1.0
        sign_s = 1.0 if sine > 0 else -1.0
        root = abs(cosine)
        return (real * sign_c + imag * sign_s) * root, (imag * sign_c - real * sign_s) * root
    return real * cosine + imag * sine, imag * cosine - real * sine


def plus(first, second):
    return first[0] + second[0], first[1] + second[1]


def minus(first, second):
    return first[0] - second[0], first[1] - second[1]


def dft_small(values):
    size = len(values)
    if size == 1:
        return values
    half = size // 2
    even = dft_small([plus(values[j], values[j + half]) for j in range(half)])
    odd = dft_small(
        [times(minus(values[j], values[j + half]), 2.0 * math.pi * j / size) for j in range(half)]
    )
    out = []
    for j in range(half):
        out += [even[j], odd[j]]
    return out


def spectra_kernel(
    frames_ref, taps_ref, twiddle_ref, high_ref, low_ref, gate_ref, out_ref,
    padded, filtered, first_half, second_half,
):
    del gate_ref
    blank = jnp.zeros((FRAMES, LANES), jnp.float32)

    def fir(a, carry):
        lane = pl.ds(pl.multiple_of(a * LANES, LANES), LANES)
        for part in range(2):
            for i in range(2):
                row = 2 * part + i
                padded[row, a, pl.ds(0, FRAMES), :] = blank
                padded[row, a, pl.ds(FRAMES, FRAMES), :] = frames_ref[part, i, :, lane].astype(
                    jnp.float32
                )
        totals = [blank] * 4
        for t in range(TAPS):
            tap = taps_ref[t, pl.ds(a, 1), :]
            for row in range(4):
                window = padded[row, a, pl.ds(FRAMES - TAPS + 1 + t, FRAMES), :]
                totals[row] = totals[row] + window * tap
        for part in range(2):
            for i in range(2):
                filtered[part, a, pl.ds(FRAMES * i, FRAMES), :] = totals[2 * part + i]
        return carry

    lax.fori_loop(0, OUTER, fir, 0)

    def load(a, i):
        rows = pl.ds(FRAMES * i, FRAMES)
        return filtered[0, a, rows, :], filtered[1, a, rows, :]

    for i in range(2):
        rows = pl.ds(FRAMES * i, FRAMES)
        for a0 in range(8):
            spread = dft_small([load(8 * a1 + a0, i) for a1 in range(4)])
            for j in range(4):
                real, imag = times(spread[j], 2.0 * math.pi * a0 * j / OUTER)
                filtered[0, 8 * j + a0, rows, :] = real
                filtered[1, 8 * j + a0, rows, :] = imag
    for i in range(2):
        for j in range(4):
            spread = dft_small([load(8 * j + a0, i) for a0 in range(8)])
            for m in range(8):
                k1 = j + 4 * m
                cosine = twiddle_ref[0, pl.ds(k1, 1), :]
                sine = twiddle_ref[1, pl.ds(k1, 1), :]
                real, imag = spread[m]
                turned_real = real * cosine + imag * sine
                turned_imag = imag * cosine - real * sine
                upper = pl.ds(4 * k1 + i, FRAMES, stride=4 * OUTER)
                lower = pl.ds(4 * k1 + 2 + i, FRAMES, stride=4 * OUTER)
                first_half[upper, :] = turned_real
                second_half[upper, :] = turned_imag
                first_half[lower, :] = turned_imag
                second_half[lower, :] = -turned_real

    block = 256

    def product(step, carry):
        rows = pl.ds(pl.multiple_of(step * block, block), block)
        left = jnp.concatenate([first_half[rows, :], second_half[rows, :]], axis=1)
        left_high = left.astype(jnp.bfloat16)
        left_low = (left - left_high.astype(jnp.float32)).astype(jnp.bfloat16)
        right_high = high_ref[...]
        total = jnp.dot(left_high, right_high, preferred_element_type=jnp.float32)
        total += jnp.dot(left_low, right_high, preferred_element_type=jnp.float32)
        total += jnp.dot(left_high, low_ref[...], preferred_element_type=jnp.float32)
        out_ref[rows, :] = total.astype(jnp.bfloat16)
        return carry

    lax.fori_loop(0, 4 * OUTER * FRAMES // block, product, 0)


def spectra_of(frames, filter_taps, gate):
    channels = frames.shape[3]
    twiddle, table = dft_tables(channels)
    high = table.astype(jnp.bfloat16)
    low = (table - high.astype(np.float32)).astype(jnp.bfloat16)
    rows = 4 * OUTER * FRAMES
    return pl.pallas_call(
        spectra_kernel,
        out_shape=jax.ShapeDtypeStruct((rows, LANES), jnp.bfloat16),
        in_specs=[pl.BlockSpec(memory_space=pltpu.VMEM)] * 5 + [pl.BlockSpec(memory_space=pl.ANY)],
        out_specs=pl.BlockSpec(memory_space=pltpu.VMEM),
        scratch_shapes=[
            pltpu.VMEM((4, OUTER, 2 * FRAMES, LANES), jnp.float32),
            pltpu.VMEM((2, OUTER, 2 * FRAMES, LANES), jnp.float32),
            pltpu.VMEM((rows, LANES), jnp.float32),
            pltpu.VMEM((rows, LANES), jnp.float32),
        ],
        compiler_params=pltpu.CompilerParams(vmem_limit_bytes=24 * 1024 * 1024),
        cost_estimate=pl.CostEstimate(
            flops=6 * rows * 256 * LANES, bytes_accessed=4 * 1024 * 1024, transcendentals=0
        ),
        name="spectra",
    )(
        frames,
        filter_taps.reshape(TAPS, OUTER, LANES),
        jnp.asarray(twiddle),
        jnp.asarray(high),
        jnp.asarray(low),
        gate,
    )


def local_weights(beam_weights, station_map, station_flags):
    beams = beam_weights.shape[1]
    inputs = beam_weights.shape[2]
    order = station_map.reshape(32, 16).T.reshape(-1)
    target = (2 * order[:, None] + jnp.arange(2, dtype=jnp.int32)[None, :]).reshape(-1)
    keep = jnp.repeat(station_flags, 2)
    rows = jnp.arange(inputs, dtype=jnp.int32)
    select = ((rows[:, None] == target[None, :]) & (keep[:, None] > 0)).astype(jnp.bfloat16)
    weight_low = (beam_weights.astype(jnp.float32) * (1.0 / 32768.0)).astype(jnp.bfloat16)
    return jnp.dot(
        weight_low.reshape(2 * beams, inputs), select, preferred_element_type=jnp.float32
    ).astype(jnp.bfloat16)


def block_power(weights, spectra, inputs_all):
    product = jnp.dot(weights, spectra, preferred_element_type=jnp.float32)
    product = product.reshape(8, 2, 16, 2, LANES)
    beam_real = product[:, 0, :, 0] - product[:, 1, :, 1]
    beam_imag = product[:, 0, :, 1] + product[:, 1, :, 0]
    return ((beam_real * beam_real + beam_imag * beam_imag) / inputs_all).astype(jnp.bfloat16)


def channel_order(received):
    by_beam = received.transpose(1, 0, 2)
    lanes = np.arange(LANES)
    keep = (lanes[:, None] // OUTER == lanes[None, :] % 4).astype(np.float32)
    pick = (np.arange(OUTER)[:, None] == lanes[None, :] // 4).astype(np.float32)
    spread = jnp.tile(by_beam, (1, 4, 1)) * jnp.asarray(keep, jnp.bfloat16)[None]
    return jnp.einsum(
        "jk,bqk->bjq", jnp.asarray(pick, jnp.bfloat16), spread, preferred_element_type=jnp.float32
    )


def on_device(voltages, filter_taps, beam_weights, station_map, station_flags):
    channels = filter_taps.shape[1]
    inputs_all = beam_weights.shape[2]
    here = lax.axis_index("stn")
    retiled = lax.all_to_all(voltages, "tm", split_axis=1, concat_axis=2, tiled=True)
    own = local_weights(beam_weights, station_map, station_flags)
    far = lax.ppermute(own, "stn", SWAP_HALF)
    upper = (here // 8) % 2 == 1
    both = jnp.concatenate([jnp.where(upper, far, own), jnp.where(upper, own, far)], axis=0)
    gathered = lax.all_gather(both, "stn", axis=0, tiled=True, axis_index_groups=QUADS)
    frames = retiled.reshape(2, 2, FRAMES, channels)
    outgoing = spectra_of(frames, filter_taps, gathered[:16, :LANES]).reshape(512, 4, LANES)
    turned = lax.all_to_all(outgoing, BOTH, split_axis=0, concat_axis=0, tiled=True)
    turned = turned.reshape(512, 2, 2, LANES).transpose(0, 2, 1, 3).reshape(inputs_all, 2 * LANES)
    other_core = lax.ppermute(gathered, "stn", SWAP_CORE)
    other_xhi = lax.ppermute(gathered, "stn", SWAP_XHI)
    other_both = lax.ppermute(other_xhi, "stn", SWAP_CORE)
    power = jnp.stack(
        [
            block_power(weights, turned, inputs_all)
            for weights in (gathered, other_core, other_xhi, other_both)
        ]
    ).reshape(2, 2, 4, 2, 16, LANES)
    power = power.transpose(0, 3, 2, 1, 4, 5)
    power = jnp.where(here % 2 == 1, power[:, :, :, ::-1], power)
    power = jnp.where(here >= 16, power[::-1], power)
    received = lax.all_to_all(power.reshape(32, 16, LANES), "stn", 0, 0, tiled=True)
    return channel_order(received).reshape(16, 1, channels)


def solution(mesh):
    placed = (P(None, "stn", "tm"), P(), P(None, "stn", None), P(), P())
    return jax.shard_map(
        on_device, mesh=mesh, in_specs=placed, out_specs=P("stn", "tm", None), check_vma=False
    )
```
